16 devices in a mesh: tp: 2 (over z), sp: 8 (over y, x, core).
Axes of the slice: x: 2, y: 2, z: 2, core: 2. Of those that a mesh axis runs over, the one named last changes fastest.
Arguments:
- x_tok: bfloat16 [256, 4096], replicated
- seq_lens: int32 [256], replicated
- k_cache: bfloat16 [256, 512, 8, 128], P(None, 'sp', 'tp')
- v_cache: bfloat16 [256, 512, 8, 128], P(None, 'sp', 'tp')
- g_attn: bfloat16 [4096], replicated
- w_q: bfloat16 [4096, 4096], P(None, 'tp')
- w_k: bfloat16 [4096, 1024], P(None, 'tp')
- w_v: bfloat16 [4096, 1024], P(None, 'tp')
- w_o: bfloat16 [4096, 4096], P('tp')
- g_mlp: bfloat16 [4096], replicated
- w_gate: bfloat16 [4096, 14336], P(None, 'tp')
- w_up: bfloat16 [4096, 14336], P(None, 'tp')
- w_down: bfloat16 [14336, 4096], P('tp')
Outputs:
- output 1: bfloat16 [256, 4096], replicated
- output 2: bfloat16 [256, 512, 8, 128], P(None, 'sp', 'tp')
- output 3: bfloat16 [256, 512, 8, 128], P(None, 'sp', 'tp')
All inputs are finite; a program needn't handle non-finite values.
Results may differ from the reference program's by a relative error of at most 0.0139779.
Values sent between devices are 32-bit elements.
A program may use at most 1.25 GiB of HBM per device.

```python
import math
import jax
import jax.numpy as jnp
from jax import lax

MODEL_DIM = 4096
Q_HEADS = 32
KV_HEADS = 8
HEAD_DIM = 128
FF_DIM = 14336
BATCH_SIZE = 256
SEQ_LEN = 512

ROPE_BASE = 500000.0
NORM_EPS = 1e-5


def gauss_draw(rng_key, arr_shape):
    return jax.random.normal(rng_key, arr_shape, jnp.float32)


def draw_lens(rng_key):
    low_len = SEQ_LEN // 4
    key_len, key_hi, key_lo = jax.random.split(rng_key, 3)
    lens_raw = jax.random.randint(key_len, (BATCH_SIZE,), low_len, SEQ_LEN)
    idx_hi = jax.random.randint(key_hi, (), 0, BATCH_SIZE)
    idx_lo = (idx_hi + jax.random.randint(key_lo, (), 1, BATCH_SIZE)) % BATCH_SIZE
    row_ids = jnp.arange(BATCH_SIZE)
    lens_raw = jnp.where(row_ids == idx_hi, SEQ_LEN - 1, lens_raw)
    lens_raw = jnp.where(row_ids == idx_lo, low_len, lens_raw)
    return lens_raw.astype(jnp.int32)


def setup_inputs(seed: int = 0) -> dict:
    key_list = jax.random.split(jax.random.key(seed), 14)
    q_width = Q_HEADS * HEAD_DIM
    kv_width = KV_HEADS * HEAD_DIM
    groups = Q_HEADS // KV_HEADS
    cache_shape = (BATCH_SIZE, SEQ_LEN, KV_HEADS, HEAD_DIM)
    w_q32 = gauss_draw(key_list[4], (MODEL_DIM, q_width)) * MODEL_DIM ** -0.5
    self_gain = (math.log(SEQ_LEN) - 0.6) * math.sqrt(groups / HEAD_DIM)
    group_sum = jnp.sum(w_q32.reshape(MODEL_DIM, KV_HEADS, groups, HEAD_DIM), axis=2).reshape(MODEL_DIM, kv_width)
    w_k32 = group_sum * (self_gain / math.sqrt(groups)) + gauss_draw(key_list[5], (MODEL_DIM, kv_width)) * (0.5 * MODEL_DIM ** -0.5)
    value_scale = 0.5 * math.sqrt(SEQ_LEN)
    return {
        "x_tok": gauss_draw(key_list[0], (BATCH_SIZE, MODEL_DIM)).astype(jnp.bfloat16),
        "seq_lens": draw_lens(key_list[1]),
        "k_cache": gauss_draw(key_list[2], cache_shape).astype(jnp.bfloat16),
        "v_cache": (gauss_draw(key_list[3], cache_shape) * value_scale).astype(jnp.bfloat16),
        "g_attn": (1.0 + 0.2 * gauss_draw(key_list[6], (MODEL_DIM,))).astype(jnp.bfloat16),
        "w_q": w_q32.astype(jnp.bfloat16),
        "w_k": w_k32.astype(jnp.bfloat16),
        "w_v": (gauss_draw(key_list[7], (MODEL_DIM, kv_width)) * MODEL_DIM ** -0.5).astype(jnp.bfloat16),
        "w_o": (gauss_draw(key_list[8], (q_width, MODEL_DIM)) * q_width ** -0.5).astype(jnp.bfloat16),
        "g_mlp": (1.0 + 0.2 * gauss_draw(key_list[9], (MODEL_DIM,))).astype(jnp.bfloat16),
        "w_gate": (gauss_draw(key_list[10], (MODEL_DIM, FF_DIM)) * MODEL_DIM ** -0.5).astype(jnp.bfloat16),
        "w_up": (gauss_draw(key_list[11], (MODEL_DIM, FF_DIM)) * MODEL_DIM ** -0.5).astype(jnp.bfloat16),
        "w_down": (gauss_draw(key_list[12], (FF_DIM, MODEL_DIM)) * FF_DIM ** -0.5).astype(jnp.bfloat16),
    }


def rms_norm(x_in, norm_gain):
    x_f32 = x_in.astype(jnp.float32)
    inv_rms = lax.rsqrt(jnp.mean(x_f32 * x_f32, axis=-1, keepdims=True) + NORM_EPS)
    return (x_f32 * inv_rms * norm_gain.astype(jnp.float32)).astype(jnp.bfloat16)


def apply_rope(heads_in, positions):
    head_dim = heads_in.shape[-1]
    half_dim = head_dim // 2
    inv_freq = jnp.power(jnp.float32(ROPE_BASE), jnp.arange(half_dim, dtype=jnp.float32) * (-2.0 / head_dim))
    angles = positions.astype(jnp.float32)[:, None, None] * inv_freq
    cos_a = jnp.cos(angles)
    sin_a = jnp.sin(angles)
    heads_f32 = heads_in.astype(jnp.float32)
    first_half = heads_f32[..., :half_dim]
    second_half = heads_f32[..., half_dim:]
    rotated = jnp.concatenate([first_half * cos_a - second_half * sin_a, second_half * cos_a + first_half * sin_a], axis=-1)
    return rotated.astype(jnp.bfloat16)


def reference(x_tok, seq_lens, k_cache, v_cache, g_attn, w_q, w_k, w_v, w_o, g_mlp, w_gate, w_up, w_down):
    groups = Q_HEADS // KV_HEADS
    x_norm = rms_norm(x_tok, g_attn)
    q_new = jnp.dot(x_norm, w_q, preferred_element_type=jnp.float32).astype(jnp.bfloat16).reshape(BATCH_SIZE, Q_HEADS, HEAD_DIM)
    k_new = jnp.dot(x_norm, w_k, preferred_element_type=jnp.float32).astype(jnp.bfloat16).reshape(BATCH_SIZE, KV_HEADS, HEAD_DIM)
    v_new = jnp.dot(x_norm, w_v, preferred_element_type=jnp.float32).astype(jnp.bfloat16).reshape(BATCH_SIZE, KV_HEADS, HEAD_DIM)
    q_rot = apply_rope(q_new, seq_lens)
    k_rot = apply_rope(k_new, seq_lens)
    row_ids = jnp.arange(BATCH_SIZE)
    k_out = k_cache.at[row_ids, seq_lens].set(k_rot)
    v_out = v_cache.at[row_ids, seq_lens].set(v_new)
    score_scale = HEAD_DIM ** -0.5

    def attend_row(row_inputs):
        q_row, k_rows, v_rows, row_len = row_inputs
        scores = jnp.einsum("kgd,tkd->kgt", q_row.astype(jnp.float32), k_rows.astype(jnp.float32)) * score_scale
        is_valid = jnp.arange(SEQ_LEN) <= row_len
        masked = jnp.where(is_valid, scores, -jnp.inf)
        row_max = jnp.max(masked, axis=-1, keepdims=True)
        weights = jnp.exp(masked - row_max)
        row_sum = jnp.sum(weights, axis=-1, keepdims=True)
        mixed = jnp.einsum("kgt,tkd->kgd", weights.astype(jnp.bfloat16).astype(jnp.float32), v_rows.astype(jnp.float32))
        return (mixed / row_sum).astype(jnp.bfloat16)

    attn_heads = lax.map(attend_row, (q_rot.reshape(BATCH_SIZE, KV_HEADS, groups, HEAD_DIM), k_out, v_out, seq_lens))
    attn_flat = attn_heads.reshape(BATCH_SIZE, Q_HEADS * HEAD_DIM)
    attn_proj = jnp.dot(attn_flat, w_o, preferred_element_type=jnp.float32)
    hidden = (x_tok.astype(jnp.float32) + attn_proj).astype(jnp.bfloat16)
    h_norm = rms_norm(hidden, g_mlp)
    gate_proj = jnp.dot(h_norm, w_gate, preferred_element_type=jnp.float32).astype(jnp.bfloat16)
    up_proj = jnp.dot(h_norm, w_up, preferred_element_type=jnp.float32).astype(jnp.bfloat16)
    act_prod = (jax.nn.silu(gate_proj.astype(jnp.float32)) * up_proj.astype(jnp.float32)).astype(jnp.bfloat16)
    mlp_out = jnp.dot(act_prod, w_down, preferred_element_type=jnp.float32)
    y_out = (hidden.astype(jnp.float32) + mlp_out).astype(jnp.bfloat16)
    return (y_out, k_out, v_out)
```

```python
import functools

import jax
import jax.numpy as jnp
from jax import lax
from jax.experimental import pallas as pl
from jax.experimental.pallas import tpu as pltpu
from jax.sharding import PartitionSpec as P

ROPE_BASE = 500000.0
NORM_EPS = 1e-5
F32 = jnp.float32
BF16 = jnp.bfloat16
MESH = pl.DeviceIdType.MESH
VMEM_LIMIT = 67_000_000

ROWS_STEP = 16
TILE_F = 256
SLOTS = 5
CUTS = ((0, 1408), (1408, 1408), (2816, 1280))


def rms_norm(x_in, norm_gain):
    x_f32 = x_in.astype(F32)
    inv_rms = lax.rsqrt(jnp.mean(x_f32 * x_f32, axis=-1, keepdims=True) + NORM_EPS)
    return (x_f32 * inv_rms * norm_gain.astype(F32)).astype(BF16)


def apply_rope(heads_in, positions):
    head_dim = heads_in.shape[-1]
    half_dim = head_dim // 2
    inv_freq = jnp.power(F32(ROPE_BASE), jnp.arange(half_dim, dtype=F32) * (-2.0 / head_dim))
    angles = positions.astype(F32)[:, None, None] * inv_freq
    cos_a = jnp.cos(angles)
    sin_a = jnp.sin(angles)
    heads_f32 = heads_in.astype(F32)
    first_half = heads_f32[..., :half_dim]
    second_half = heads_f32[..., half_dim:]
    rotated = jnp.concatenate([first_half * cos_a - second_half * sin_a, second_half * cos_a + first_half * sin_a], axis=-1)
    return rotated.astype(BF16)


def attn_kernel(pos_ref, q_ref, kn_ref, vn_ref, k_ref, v_ref, ko_ref, vo_ref, o_ref, ml_ref):
    step = pl.program_id(0)
    rows = k_ref.shape[1]
    heads = q_ref.shape[1]
    kv = rows // 64
    group = heads // kv
    scale = q_ref.shape[2] ** -0.5
    part = step % (64 // ROWS_STEP)

    row16 = lax.broadcasted_iota(jnp.int32, (16, 128), 0)
    for b in range(ROWS_STEP):
        pos = pos_ref[step * ROWS_STEP + b]
        first = pos * kv
        start = pl.multiple_of(jnp.clip(first // 16, 0, rows // 16 - 1) * 16, 16)
        lo = first - start
        here = (row16 >= lo) & (row16 < lo + kv)
        ko_ref[b] = k_ref[b]
        vo_ref[b] = v_ref[b]
        ko_ref[b, pl.ds(start, 16), :] = jnp.where(here, kn_ref[b], k_ref[b, pl.ds(start, 16), :])
        vo_ref[b, pl.ds(start, 16), :] = jnp.where(here, vn_ref[b], v_ref[b, pl.ds(start, 16), :])

    @pl.when(part == 0)
    def _():
        ml_ref[...] = jnp.zeros_like(ml_ref)

    row_id = lax.broadcasted_iota(jnp.int32, (heads, rows), 0)
    col_id = lax.broadcasted_iota(jnp.int32, (heads, rows), 1)
    same_head = (col_id % kv) == (row_id // group)
    lane = lax.broadcasted_iota(jnp.int32, (heads, 128), 1)
    maxes = jnp.concatenate([ml_ref[0, 0, 0], ml_ref[0, 1, 0]], axis=0)
    sums = jnp.concatenate([ml_ref[0, 0, 1], ml_ref[0, 1, 1]], axis=0)
    for base in range(0, ROWS_STEP, 8):
        scores, stats = [], []
        for b in range(base, base + 8):
            s = lax.dot_general(q_ref[b], ko_ref[b], (((1,), (1,)), ((), ())), preferred_element_type=F32)
            scores.append(s * scale)
        for k, b in enumerate(range(base, base + 8)):
            pos = pos_ref[step * ROWS_STEP + b]
            valid = same_head & (col_id < (pos + 1) * kv)
            s = jnp.where(valid, scores[k], -1e30)
            m = jnp.max(s, axis=1, keepdims=True)
            w = jnp.where(valid, jnp.exp(s - m), 0.0)
            total = jnp.sum(w, axis=1, keepdims=True)
            at = lane == part * ROWS_STEP + b
            maxes = jnp.where(at, m, maxes)
            sums = jnp.where(at, total, sums)
            stats.append(w.astype(BF16))
        for k, b in enumerate(range(base, base + 8)):
            o = jnp.dot(stats[k], vo_ref[b], preferred_element_type=F32)
            o_ref[0, 0, b] = o[:8]
            o_ref[0, 1, b] = o[8:]
    ml_ref[0, 0, 0] = maxes[:8]
    ml_ref[0, 1, 0] = maxes[8:]
    ml_ref[0, 0, 1] = sums[:8]
    ml_ref[0, 1, 1] = sums[8:]


def attention(pos, q, kn, vn, k_blk, v_blk):
    batch, rows, dim = k_blk.shape
    heads = q.shape[1]
    steps = batch // ROWS_STEP
    per = 64 // ROWS_STEP
    small = pl.BlockSpec((ROWS_STEP, 16, dim), lambda t, *_: (t, 0, 0))
    cache = pl.BlockSpec((ROWS_STEP, rows, dim), lambda t, *_: (t, 0, 0))
    return pl.pallas_call(
        attn_kernel,
        name="attend",
        grid_spec=pltpu.PrefetchScalarGridSpec(
            num_scalar_prefetch=1,
            grid=(steps,),
            in_specs=[small, small, small, cache, cache],
            out_specs=[
                cache,
                cache,
                pl.BlockSpec((1, 2, ROWS_STEP, 8, dim), lambda t, *_: (t // per, 0, t % per, 0, 0)),
                pl.BlockSpec((1, 2, 2, 8, dim), lambda t, *_: (t // per, 0, 0, 0, 0)),
            ],
        ),
        out_shape=[
            jax.ShapeDtypeStruct(k_blk.shape, BF16),
            jax.ShapeDtypeStruct(v_blk.shape, BF16),
            jax.ShapeDtypeStruct((batch // 64, 2, 64, 8, dim), F32),
            jax.ShapeDtypeStruct((batch // 64, 2, 2, 8, dim), F32),
        ],
        cost_estimate=pl.CostEstimate(flops=4 * batch * heads * rows * dim, bytes_accessed=8 * batch * rows * dim, transcendentals=batch * heads * rows),
    )(pos, q, kn, vn, k_blk, v_blk)


def blend(pairs, out_ref):
    for b in range(64):
        total = None
        for weight, part in pairs:
            term = jnp.broadcast_to(weight[:, b : b + 1], (8, 128)) * part[b]
            total = term if total is None else total + term
        out_ref[b] = total


def tail_kernel(o_ref, ml_ref, x_ref, g_ref, wo_hbm, wg_hbm, wu_hbm, wd_hbm, y_ref,
                r1, rm1, snd, sndm, r2, rm2, attn, attn_bf, wo_v, part_o, got_o, sum_o, got_z, hid, zb,
                wg_v, wu_v, wd_v, acc, got_a, sum_a, got_b, yall,
                wo_sem, w_sem, s1, t1, s2, t2, so, to, sa, ta, sg, tg, sd, td):
    sp = lax.axis_index("sp")
    z = lax.axis_index("tp")
    c = sp % 2
    xx = (sp // 2) % 2
    yy = sp // 4
    chip = sp // 2
    depth = attn_bf.shape[1]
    width = wg_hbm.shape[1] // 2
    tiles = width // TILE_F

    wo_copy = pltpu.make_async_copy(wo_hbm.at[pl.ds(pl.multiple_of(c * depth, depth), depth), :], wo_v, wo_sem)
    wo_copy.start()

    def weight_copies(t, slot):
        at = pl.ds(pl.multiple_of(c * width + t * TILE_F, TILE_F), TILE_F)
        return (
            pltpu.make_async_copy(wg_hbm.at[:, at], wg_v.at[slot], w_sem.at[0, slot]),
            pltpu.make_async_copy(wu_hbm.at[:, at], wu_v.at[slot], w_sem.at[1, slot]),
            pltpu.make_async_copy(wd_hbm.at[at, :], wd_v.at[slot], w_sem.at[2, slot]),
        )

    for t in range(SLOTS):
        for copy in weight_copies(t, t):
            copy.start()

    def spi(fx, fy, fc):
        px = 1 - xx if fx else xx
        py = 1 - yy if fy else yy
        pc = 1 - c if fc else c
        return (py * 2 + px) * 2 + pc

    core_id = {"sp": spi(0, 0, 1)}
    x_id = {"sp": spi(1, 0, 0)}
    y_id = {"sp": spi(0, 1, 0)}
    d_id = {"sp": spi(1, 1, 0)}
    z_id = {"tp": 1 - z}

    barrier = pltpu.get_barrier_semaphore()
    for peer in (core_id, x_id, y_id, d_id, z_id):
        pl.semaphore_signal(barrier, inc=1, device_id=peer, device_id_type=MESH)
    pl.semaphore_wait(barrier, 5)

    def send(src, dst, send_sem, recv_sem, peer):
        return pltpu.make_async_remote_copy(src_ref=src, dst_ref=dst, send_sem=send_sem, recv_sem=recv_sem, device_id=peer, device_id_type=MESH)

    groups = [(1 - yy) * 2 + (1 - xx), yy * 2 + (1 - xx), (1 - yy) * 2 + xx, chip]
    peers = [d_id, x_id, y_id]
    first = []
    for k in range(4):
        a = send(o_ref.at[groups[k], 1 - c], r1.at[k], s1.at[0, k], t1.at[0, k], core_id)
        b = send(ml_ref.at[groups[k], 1 - c], rm1.at[k], s1.at[1, k], t1.at[1, k], core_id)
        a.start()
        b.start()
        first.append((a, b))
    second = []
    for k in range(4):
        for copy in first[k]:
            copy.wait_recv()
        m0, l0 = ml_ref[groups[k], c, 0], ml_ref[groups[k], c, 1]
        m1, l1 = rm1[k, 0], rm1[k, 1]
        m = jnp.maximum(m0, m1)
        f0, f1 = jnp.exp(m0 - m), jnp.exp(m1 - m)
        sndm[k, 0] = m
        sndm[k, 1] = f0 * l0 + f1 * l1
        blend([(f0, o_ref.at[groups[k], c]), (f1, r1.at[k])], snd.at[k])
        if k < 3:
            a = send(snd.at[k], r2.at[k], s2.at[0, k], t2.at[0, k], peers[k])
            b = send(sndm.at[k], rm2.at[k], s2.at[1, k], t2.at[1, k], peers[k])
            a.start()
            b.start()
            second.append((a, b))
    for k in (1, 2, 0):
        for copy in second[k]:
            copy.wait_recv()
    ms = [sndm[3, 0]] + [rm2[k, 0] for k in range(3)]
    ls = [sndm[3, 1]] + [rm2[k, 1] for k in range(3)]
    m = functools.reduce(jnp.maximum, ms)
    fs = [jnp.exp(v - m) for v in ms]
    total = fs[0] * ls[0] + fs[1] * ls[1] + fs[2] * ls[2] + fs[3] * ls[3]
    total = jnp.where(total > 0.0, total, 1.0)
    blend([(fs[0] / total, snd.at[3])] + [(fs[k + 1] / total, r2.at[k]) for k in range(3)], attn)
    for h in range(8):
        attn_bf[:, h * 128 : (h + 1) * 128] = attn[:, h, :].astype(BF16)

    wo_copy.wait()

    def wo_step(n, carry):
        at = pl.ds(pl.multiple_of(n * 512, 512), 512)
        part_o[:, at] = jnp.dot(attn_bf[...], wo_v[:, at], preferred_element_type=F32)
        return carry

    lax.fori_loop(0, part_o.shape[1] // 512, wo_step, 0)
    mine = pl.ds(pl.multiple_of(c * 32, 32), 32)
    other = pl.ds(pl.multiple_of((1 - c) * 32, 32), 32)
    copy_o = send(part_o.at[other], got_o, so.at[0], to.at[0], core_id)
    copy_o.start()
    copy_o.wait_recv()
    sum_o[...] = part_o[mine] + got_o[...]
    copy_z = send(sum_o, got_z, so.at[1], to.at[1], z_id)
    copy_z.start()
    copy_z.wait_recv()
    x_rows = x_ref[pl.ds(pl.multiple_of(chip * 64 + c * 32, 32), 32), :].astype(F32)
    hid[mine] = (x_rows + (sum_o[...] + got_z[...])).astype(BF16).astype(F32)
    copy_h = send(hid.at[mine], hid.at[mine], so.at[2], to.at[2], core_id)
    copy_h.start()
    copy_h.wait_recv()

    h = hid[...]
    r = lax.rsqrt(jnp.mean(h * h, axis=-1, keepdims=True) + NORM_EPS)
    zb[...] = (h * r * g_ref[...].astype(F32)).astype(BF16)
    acc[...] = jnp.zeros_like(acc)

    def mlp_step(t, carry):
        slot = lax.rem(t, SLOTS)
        for copy in weight_copies(t, slot):
            copy.wait()
        gate = jnp.dot(zb[...], wg_v[slot], preferred_element_type=F32).astype(BF16).astype(F32)
        up = jnp.dot(zb[...], wu_v[slot], preferred_element_type=F32).astype(BF16).astype(F32)
        act = (gate * jax.nn.sigmoid(gate) * up).astype(BF16)
        acc[...] += jnp.dot(act, wd_v[slot], preferred_element_type=F32)

        @pl.when(t + SLOTS < tiles)
        def _():
            for copy in weight_copies(t + SLOTS, slot):
                copy.start()

        return carry

    lax.fori_loop(0, tiles, mlp_step, 0)

    copy_a = send(acc.at[other], got_a, sa.at[0], ta.at[0], core_id)
    copy_a.start()
    copy_a.wait_recv()
    sum_a[...] = acc[mine] + got_a[...]
    zmine = pl.ds(pl.multiple_of(z * 16, 16), 16)
    zother = pl.ds(pl.multiple_of((1 - z) * 16, 16), 16)
    copy_b = send(sum_a.at[zother], got_b, sa.at[1], ta.at[1], z_id)
    copy_b.start()
    copy_b.wait_recv()

    def rows_of(flips, fc=0):
        px = 1 - xx if "x" in flips else xx
        py = 1 - yy if "y" in flips else yy
        pz = 1 - z if "z" in flips else z
        pc = 1 - c if fc else c
        block = ((py * 2 + px) * 2 + pc) * 2 + pz
        return pl.ds(pl.multiple_of(block * 16, 16), 16)

    hid16 = hid[pl.ds(pl.multiple_of(c * 32 + z * 16, 16), 16), :]
    yall[rows_of("")] = (hid16 + (sum_a[zmine] + got_b[...])).astype(BF16).astype(F32)

    ids = {"x": x_id, "y": y_id, "z": z_id}
    orders = ("xyz", "yzx", "zxy")

    def gather_copy(p, idx):
        d0, d1, d2 = orders[p]
        src = ["", "", d0, "", d0, d1, d0 + d1][idx]
        to_dim = [d0, d1, d1, d2, d2, d2, d2][idx]
        ref = yall.at[rows_of(src), pl.ds(*CUTS[p])]
        return send(ref, ref, sg.at[p, idx], tg.at[p, idx], ids[to_dim])

    def landed(p, idx):
        d0, d1, d2 = orders[p]
        return [d0, d1, d0 + d1, d2, d2 + d0, d2 + d1, d0 + d1 + d2][idx]

    def gather_wait(p, idx):
        ref = yall.at[rows_of(landed(p, idx)), pl.ds(*CUTS[p])]
        send(ref, ref, sg.at[p, idx], tg.at[p, idx], core_id).wait_recv()

    def core_copy(p, j):
        flips = "" if j == 0 else landed(p, j - 1)
        ref = yall.at[rows_of(flips), pl.ds(*CUTS[p])]
        return send(ref, ref, sd.at[p, j], td.at[p, j], core_id)

    for idx in (0, 1, 3):
        for p in range(3):
            gather_copy(p, idx).start()
    for p in range(3):
        core_copy(p, 0).start()
    for p in range(3):
        gather_wait(p, 0)
        gather_copy(p, 2).start()
        gather_copy(p, 4).start()
        core_copy(p, 1).start()
    for p in range(3):
        gather_wait(p, 1)
        gather_copy(p, 5).start()
        core_copy(p, 2).start()
    for p in range(3):
        gather_wait(p, 2)
        gather_copy(p, 6).start()
        core_copy(p, 3).start()
    for idx in (3, 4, 5, 6):
        for p in range(3):
            gather_wait(p, idx)
            core_copy(p, idx + 1).start()
    for p in range(3):
        for j in range(8):
            flips = "" if j == 0 else landed(p, j - 1)
            ref = yall.at[rows_of(flips, 1), pl.ds(*CUTS[p])]
            send(ref, ref, sd.at[p, j], td.at[p, j], core_id).wait_recv()
    y_ref[...] = yall[...].astype(BF16)

    for pair in first + second:
        for copy in pair:
            copy.wait_send()
    for copy in (copy_o, copy_z, copy_h, copy_a, copy_b):
        copy.wait_send()
    for p in range(3):
        for idx in range(7):
            gather_copy(p, idx).wait_send()
        for j in range(8):
            core_copy(p, j).wait_send()


def tail(o, ml, x_tok, g_mlp, wo, wg, wu, wd):
    batch, width = x_tok.shape
    depth = wo.shape[0] // 2
    vmem = pl.BlockSpec(memory_space=pltpu.VMEM)
    hbm = pl.BlockSpec(memory_space=pl.ANY)
    dma = pltpu.SemaphoreType.DMA
    heads = (64, 8, 128)
    stat = (2, 8, 128)
    return pl.pallas_call(
        tail_kernel,
        name="tail",
        out_shape=jax.ShapeDtypeStruct((batch, width), BF16),
        in_specs=[vmem, vmem, vmem, vmem, hbm, hbm, hbm, hbm],
        out_specs=vmem,
        scratch_shapes=[
            pltpu.VMEM((4, *heads), F32), pltpu.VMEM((4, *stat), F32),
            pltpu.VMEM((4, *heads), F32), pltpu.VMEM((4, *stat), F32),
            pltpu.VMEM((3, *heads), F32), pltpu.VMEM((3, *stat), F32),
            pltpu.VMEM(heads, F32), pltpu.VMEM((64, depth), BF16),
            pltpu.VMEM((depth, width), BF16), pltpu.VMEM((64, width), F32),
            pltpu.VMEM((32, width), F32), pltpu.VMEM((32, width), F32), pltpu.VMEM((32, width), F32),
            pltpu.VMEM((64, width), F32), pltpu.VMEM((64, width), BF16),
            pltpu.VMEM((SLOTS, width, TILE_F), BF16), pltpu.VMEM((SLOTS, width, TILE_F), BF16), pltpu.VMEM((SLOTS, TILE_F, width), BF16),
            pltpu.VMEM((64, width), F32), pltpu.VMEM((32, width), F32), pltpu.VMEM((32, width), F32), pltpu.VMEM((16, width), F32),
            pltpu.VMEM((batch, width), F32),
            dma, dma((3, SLOTS)), dma((2, 4)), dma((2, 4)), dma((2, 3)), dma((2, 3)),
            dma((3,)), dma((3,)), dma((2,)), dma((2,)), dma((3, 7)), dma((3, 7)), dma((3, 8)), dma((3, 8)),
        ],
        compiler_params=pltpu.CompilerParams(collective_id=0, has_side_effects=True, vmem_limit_bytes=VMEM_LIMIT),
        cost_estimate=pl.CostEstimate(flops=10**10, bytes_accessed=10**8, transcendentals=0),
    )(o, ml, x_tok, g_mlp, wo, wg, wu, wd)


def solution(mesh):
    cache_spec = P(None, "sp", "tp", None)
    col_spec = P(None, "tp")
    row_spec = P("tp", None)
    full_spec = P()

    def local_step(x_tok, seq_lens, k_blk, v_blk, g_attn, wq_loc, wk_loc, wv_loc, wo_loc, g_mlp, wg_loc, wu_loc, wd_loc):
        batch_rows, seq_blk, kv_loc, head_dim = k_blk.shape
        q_loc = wq_loc.shape[1] // head_dim
        x_norm = rms_norm(x_tok, g_attn)
        q_new = jnp.dot(x_norm, wq_loc, preferred_element_type=F32).astype(BF16).reshape(batch_rows, q_loc, head_dim)
        k_new = jnp.dot(x_norm, wk_loc, preferred_element_type=F32).astype(BF16).reshape(batch_rows, kv_loc, head_dim)
        v_new = jnp.dot(x_norm, wv_loc, preferred_element_type=F32).astype(BF16).reshape(batch_rows, kv_loc, head_dim)
        q_rot = apply_rope(q_new, seq_lens)
        k_rot = apply_rope(k_new, seq_lens)
        pos = seq_lens - lax.axis_index("sp") * seq_blk
        reps = 16 // kv_loc
        flat = (batch_rows, seq_blk * kv_loc, head_dim)
        k_out, v_out, o, ml = attention(
            pos, q_rot, jnp.tile(k_rot, (1, reps, 1)), jnp.tile(v_new, (1, reps, 1)), k_blk.reshape(flat), v_blk.reshape(flat)
        )
        y_out = tail(o, ml, x_tok, g_mlp.reshape(1, -1), wo_loc, wg_loc, wu_loc, wd_loc)
        return y_out, k_out.reshape(k_blk.shape), v_out.reshape(v_blk.shape)

    return jax.shard_map(local_step, mesh=mesh, in_specs=(full_spec, full_spec, cache_spec, cache_spec, full_spec, col_spec, col_spec, col_spec, row_spec, full_spec, col_spec, col_spec, row_spec), out_specs=(full_spec, cache_spec, cache_spec), check_vma=False)
```

```python
import functools

import jax
import jax.numpy as jnp
from jax import lax
from jax.experimental import pallas as pl
from jax.experimental.pallas import tpu as pltpu
from jax.sharding import PartitionSpec as P

ROPE_BASE = 500000.0
NORM_EPS = 1e-5
F32 = jnp.float32
BF16 = jnp.bfloat16
MESH = pl.DeviceIdType.MESH
VMEM_LIMIT = 67_000_000

ROWS_STEP = 16
TILE_F = 256
RING = 6
SLOTS = 5
CUTS = ((0, 1408), (1408, 1408), (2816, 1280))


def front_kernel(pos_ref, x_ref, g_ref, cos_ref, sin_ref, wq_hbm, wk_hbm, wv_hbm, k_hbm, v_hbm,
                 ko_hbm, vo_hbm, o_ref, ml_ref, xn, w_v, qf, kf, vf, kbuf, vbuf, w_sem, in_sem, out_sem):
    batch = x_ref.shape[0]
    rows, dim = k_hbm.shape[1:]
    kv = rows // 64
    heads = wq_hbm.shape[1] // dim
    group = heads // kv
    scale = dim**-0.5
    steps = batch // ROWS_STEP
    q_tiles, k_tiles = wq_hbm.shape[1] // 256, wk_hbm.shape[1] // 256

    weights = [(wq_hbm, j) for j in range(q_tiles)] + [(wk_hbm, j) for j in range(k_tiles)] + [(wv_hbm, j) for j in range(k_tiles)]
    for t, (ref, j) in enumerate(weights):
        pltpu.make_async_copy(ref.at[:, pl.ds(j * 256, 256)], w_v.at[t], w_sem.at[t]).start()

    def block_in(t, slot):
        at = pl.ds(pl.multiple_of(t * ROWS_STEP, ROWS_STEP), ROWS_STEP)
        return (
            pltpu.make_async_copy(k_hbm.at[at], kbuf.at[slot], in_sem.at[0, slot]),
            pltpu.make_async_copy(v_hbm.at[at], vbuf.at[slot], in_sem.at[1, slot]),
        )

    def block_out(t, slot):
        at = pl.ds(pl.multiple_of(t * ROWS_STEP, ROWS_STEP), ROWS_STEP)
        return (
            pltpu.make_async_copy(kbuf.at[slot], ko_hbm.at[at], out_sem.at[0, slot]),
            pltpu.make_async_copy(vbuf.at[slot], vo_hbm.at[at], out_sem.at[1, slot]),
        )

    for t in range(RING):
        for copy in block_in(t, t):
            copy.start()

    def norm_step(j, carry):
        at = pl.ds(pl.multiple_of(j * 32, 32), 32)
        x = x_ref[at, :].astype(F32)
        r = lax.rsqrt(jnp.mean(x * x, axis=-1, keepdims=True) + NORM_EPS)
        xn[at, :] = (x * r * g_ref[...].astype(F32)).astype(BF16)
        return carry

    lax.fori_loop(0, batch // 32, norm_step, 0)

    def project(t):
        pltpu.make_async_copy(wk_hbm.at[:, pl.ds(0, 256)], w_v.at[t], w_sem.at[t]).wait()
        return jnp.dot(xn[...], w_v[t], preferred_element_type=F32).astype(BF16).astype(F32)

    def rotate(head):
        return (head * cos_ref[...] + pltpu.roll(head, dim // 2, 1) * sin_ref[...]).astype(BF16).astype(F32)

    def q_step(t, carry):
        y = project(t)
        for j in range(2):
            qf[pl.ds(2 * t + j, batch, stride=heads), :] = rotate(y[:, j * dim : (j + 1) * dim])
        return carry

    def k_step(t, carry):
        y = project(q_tiles + t)
        for j in range(2):
            head = rotate(y[:, j * dim : (j + 1) * dim])
            for rep in range(16 // kv):
                kf[pl.ds(rep * kv + 2 * t + j, batch, stride=16), :] = head
        return carry

    def v_step(t, carry):
        y = project(q_tiles + k_tiles + t)
        for j in range(2):
            for rep in range(16 // kv):
                vf[pl.ds(rep * kv + 2 * t + j, batch, stride=16), :] = y[:, j * dim : (j + 1) * dim]
        return carry

    lax.fori_loop(0, q_tiles, q_step, 0)
    lax.fori_loop(0, k_tiles, k_step, 0)
    lax.fori_loop(0, k_tiles, v_step, 0)

    ml_ref[...] = jnp.zeros_like(ml_ref)
    row16 = lax.broadcasted_iota(jnp.int32, (16, dim), 0)
    row_id = lax.broadcasted_iota(jnp.int32, (heads, rows), 0)
    col_id = lax.broadcasted_iota(jnp.int32, (heads, rows), 1)
    same_head = (col_id % kv) == (row_id // group)
    col_id = jnp.where(same_head, col_id, rows * 1024)
    lane = lax.broadcasted_iota(jnp.int32, (heads, 128), 1)
    per = 64 // ROWS_STEP

    def attend_step(t, carry):
        slot = lax.rem(t, RING)
        chip, part = lax.div(t, per), lax.rem(t, per)
        for copy in block_in(t, slot):
            copy.wait()
        for b in range(ROWS_STEP):
            first = pos_ref[t * ROWS_STEP + b] * kv
            start = pl.multiple_of(jnp.clip(first // 16, 0, rows // 16 - 1) * 16, 16)
            lo = first - start
            here = (row16 >= lo) & (row16 < lo + kv)
            new = pl.ds(pl.multiple_of((t * ROWS_STEP + b) * 16, 16), 16)
            at = pl.ds(start, 16)
            kbuf[slot, b, at, :] = jnp.where(here, kf[new, :].astype(BF16), kbuf[slot, b, at, :])
            vbuf[slot, b, at, :] = jnp.where(here, vf[new, :].astype(BF16), vbuf[slot, b, at, :])
        maxes = jnp.concatenate([ml_ref[chip, 0, 0], ml_ref[chip, 1, 0]], axis=0)
        sums = jnp.concatenate([ml_ref[chip, 0, 1], ml_ref[chip, 1, 1]], axis=0)
        for base in range(0, ROWS_STEP, 8):
            scores, weights = [], []
            for b in range(base, base + 8):
                q = qf[pl.ds(pl.multiple_of((t * ROWS_STEP + b) * heads, heads), heads), :].astype(BF16)
                s = lax.dot_general(q, kbuf[slot, b], (((1,), (1,)), ((), ())), preferred_element_type=F32)
                scores.append(s * scale)
            for n, b in enumerate(range(base, base + 8)):
                valid = col_id < (pos_ref[t * ROWS_STEP + b] + 1) * kv
                s = jnp.where(valid, scores[n], -1e30)
                m = jnp.max(s, axis=1, keepdims=True)
                w = jnp.where(valid, jnp.exp(s - m), 0.0)
                here = lane == part * ROWS_STEP + b
                maxes = jnp.where(here, m, maxes)
                sums = jnp.where(here, jnp.sum(w, axis=1, keepdims=True), sums)
                weights.append(w.astype(BF16))
            for n, b in enumerate(range(base, base + 8)):
                o = jnp.dot(weights[n], vbuf[slot, b], preferred_element_type=F32)
                o_ref[chip, 0, part * ROWS_STEP + b] = o[:8]
                o_ref[chip, 1, part * ROWS_STEP + b] = o[8:]
        ml_ref[chip, 0, 0] = maxes[:8]
        ml_ref[chip, 1, 0] = maxes[8:]
        ml_ref[chip, 0, 1] = sums[:8]
        ml_ref[chip, 1, 1] = sums[8:]
        for copy in block_out(t, slot):
            copy.start()

        @pl.when((t >= 1) & (t - 1 + RING < steps))
        def _():
            before = lax.rem(t - 1, RING)
            for copy in block_out(t - 1, before):
                copy.wait()
            for copy in block_in(t - 1 + RING, before):
                copy.start()

        return carry

    lax.fori_loop(0, steps, attend_step, 0)
    for t in range(steps - RING, steps):
        for copy in block_out(t, t % RING):
            copy.wait()


def front(pos, x_tok, g_attn, cos2, sin2, wq, wk, wv, k_blk, v_blk):
    batch, width = x_tok.shape
    _, rows, dim = k_blk.shape
    heads = wq.shape[1] // dim
    tiles = (wq.shape[1] + wk.shape[1] + wv.shape[1]) // 256
    vmem = pl.BlockSpec(memory_space=pltpu.VMEM)
    hbm = pl.BlockSpec(memory_space=pl.ANY)
    dma = pltpu.SemaphoreType.DMA
    return pl.pallas_call(
        front_kernel,
        name="front",
        in_specs=[pl.BlockSpec(memory_space=pltpu.SMEM), vmem, vmem, vmem, vmem, hbm, hbm, hbm, hbm, hbm],
        out_specs=[hbm, hbm, vmem, vmem],
        out_shape=[
            jax.ShapeDtypeStruct(k_blk.shape, BF16),
            jax.ShapeDtypeStruct(v_blk.shape, BF16),
            jax.ShapeDtypeStruct((batch // 64, 2, 64, 8, dim), F32),
            jax.ShapeDtypeStruct((batch // 64, 2, 2, 8, dim), F32),
        ],
        scratch_shapes=[
            pltpu.VMEM((batch, width), BF16),
            pltpu.VMEM((tiles, width, 256), BF16),
            pltpu.VMEM((batch * heads, dim), F32), pltpu.VMEM((batch * 16, dim), F32), pltpu.VMEM((batch * 16, dim), F32),
            pltpu.VMEM((RING, ROWS_STEP, rows, dim), BF16), pltpu.VMEM((RING, ROWS_STEP, rows, dim), BF16),
            dma((tiles,)), dma((2, RING)), dma((2, RING)),
        ],
        compiler_params=pltpu.CompilerParams(vmem_limit_bytes=VMEM_LIMIT),
        cost_estimate=pl.CostEstimate(flops=10**10, bytes_accessed=10**8, transcendentals=0),
    )(pos, x_tok, g_attn, cos2, sin2, wq, wk, wv, k_blk, v_blk)


def blend(pairs, out_ref):
    for b in range(64):
        total = None
        for weight, part in pairs:
            term = jnp.broadcast_to(weight[:, b : b + 1], (8, 128)) * part[b]
            total = term if total is None else total + term
        out_ref[b] = total


def tail_kernel(o_ref, ml_ref, x_ref, g_ref, wo_hbm, wg_hbm, wu_hbm, wd_hbm, y_ref,
                r1, rm1, snd, sndm, r2, rm2, attn, attn_bf, wo_v, part_o, got_o, sum_o, got_z, hid, zb,
                wg_v, wu_v, wd_v, acc, got_a, sum_a, got_b, yall,
                wo_sem, w_sem, s1, t1, s2, t2, so, to, sa, ta, sg, tg, sd, td):
    sp = lax.axis_index("sp")
    z = lax.axis_index("tp")
    c = sp % 2
    xx = (sp // 2) % 2
    yy = sp // 4
    chip = sp // 2
    depth = attn_bf.shape[1]
    width = wg_hbm.shape[1] // 2
    tiles = width // TILE_F

    wo_copy = pltpu.make_async_copy(wo_hbm.at[pl.ds(pl.multiple_of(c * depth, depth), depth), :], wo_v, wo_sem)
    wo_copy.start()

    def weight_copies(t, slot):
        at = pl.ds(pl.multiple_of(c * width + t * TILE_F, TILE_F), TILE_F)
        return (
            pltpu.make_async_copy(wg_hbm.at[:, at], wg_v.at[slot], w_sem.at[0, slot]),
            pltpu.make_async_copy(wu_hbm.at[:, at], wu_v.at[slot], w_sem.at[1, slot]),
            pltpu.make_async_copy(wd_hbm.at[at, :], wd_v.at[slot], w_sem.at[2, slot]),
        )

    for t in range(SLOTS):
        for copy in weight_copies(t, t):
            copy.start()

    def spi(fx, fy, fc):
        px = 1 - xx if fx else xx
        py = 1 - yy if fy else yy
        pc = 1 - c if fc else c
        return (py * 2 + px) * 2 + pc

    core_id = {"sp": spi(0, 0, 1)}
    x_id = {"sp": spi(1, 0, 0)}
    y_id = {"sp": spi(0, 1, 0)}
    d_id = {"sp": spi(1, 1, 0)}
    z_id = {"tp": 1 - z}

    barrier = pltpu.get_barrier_semaphore()
    for peer in (core_id, x_id, y_id, d_id, z_id):
        pl.semaphore_signal(barrier, inc=1, device_id=peer, device_id_type=MESH)
    pl.semaphore_wait(barrier, 5)

    def send(src, dst, send_sem, recv_sem, peer):
        return pltpu.make_async_remote_copy(src_ref=src, dst_ref=dst, send_sem=send_sem, recv_sem=recv_sem, device_id=peer, device_id_type=MESH)

    groups = [(1 - yy) * 2 + (1 - xx), yy * 2 + (1 - xx), (1 - yy) * 2 + xx, chip]
    peers = [d_id, x_id, y_id]
    first = []
    for k in range(4):
        a = send(o_ref.at[groups[k], 1 - c], r1.at[k], s1.at[0, k], t1.at[0, k], core_id)
        b = send(ml_ref.at[groups[k], 1 - c], rm1.at[k], s1.at[1, k], t1.at[1, k], core_id)
        a.start()
        b.start()
        first.append((a, b))
    second = []
    for k in range(4):
        for copy in first[k]:
            copy.wait_recv()
        m0, l0 = ml_ref[groups[k], c, 0], ml_ref[groups[k], c, 1]
        m1, l1 = rm1[k, 0], rm1[k, 1]
        m = jnp.maximum(m0, m1)
        f0, f1 = jnp.exp(m0 - m), jnp.exp(m1 - m)
        sndm[k, 0] = m
        sndm[k, 1] = f0 * l0 + f1 * l1
        blend([(f0, o_ref.at[groups[k], c]), (f1, r1.at[k])], snd.at[k])
        if k < 3:
            a = send(snd.at[k], r2.at[k], s2.at[0, k], t2.at[0, k], peers[k])
            b = send(sndm.at[k], rm2.at[k], s2.at[1, k], t2.at[1, k], peers[k])
            a.start()
            b.start()
            second.append((a, b))
    for k in (1, 2, 0):
        for copy in second[k]:
            copy.wait_recv()
    ms = [sndm[3, 0]] + [rm2[k, 0] for k in range(3)]
    ls = [sndm[3, 1]] + [rm2[k, 1] for k in range(3)]
    m = functools.reduce(jnp.maximum, ms)
    fs = [jnp.exp(v - m) for v in ms]
    total = fs[0] * ls[0] + fs[1] * ls[1] + fs[2] * ls[2] + fs[3] * ls[3]
    total = jnp.where(total > 0.0, total, 1.0)
    blend([(fs[0] / total, snd.at[3])] + [(fs[k + 1] / total, r2.at[k]) for k in range(3)], attn)
    for h in range(8):
        attn_bf[:, h * 128 : (h + 1) * 128] = attn[:, h, :].astype(BF16)

    wo_copy.wait()

    def wo_step(n, carry):
        at = pl.ds(pl.multiple_of(n * 512, 512), 512)
        part_o[:, at] = jnp.dot(attn_bf[...], wo_v[:, at], preferred_element_type=F32)
        return carry

    lax.fori_loop(0, part_o.shape[1] // 512, wo_step, 0)
    mine = pl.ds(pl.multiple_of(c * 32, 32), 32)
    other = pl.ds(pl.multiple_of((1 - c) * 32, 32), 32)
    copy_o = send(part_o.at[other], got_o, so.at[0], to.at[0], core_id)
    copy_o.start()
    copy_o.wait_recv()
    sum_o[...] = part_o[mine] + got_o[...]
    copy_z = send(sum_o, got_z, so.at[1], to.at[1], z_id)
    copy_z.start()
    copy_z.wait_recv()
    x_rows = x_ref[pl.ds(pl.multiple_of(chip * 64 + c * 32, 32), 32), :].astype(F32)
    hid[mine] = (x_rows + (sum_o[...] + got_z[...])).astype(BF16).astype(F32)
    copy_h = send(hid.at[mine], hid.at[mine], so.at[2], to.at[2], core_id)
    copy_h.start()
    copy_h.wait_recv()

    h = hid[...]
    r = lax.rsqrt(jnp.mean(h * h, axis=-1, keepdims=True) + NORM_EPS)
    zb[...] = (h * r * g_ref[...].astype(F32)).astype(BF16)
    acc[...] = jnp.zeros_like(acc)

    def mlp_step(t, carry):
        slot = lax.rem(t, SLOTS)
        for copy in weight_copies(t, slot):
            copy.wait()
        gate = jnp.dot(zb[...], wg_v[slot], preferred_element_type=F32).astype(BF16).astype(F32)
        up = jnp.dot(zb[...], wu_v[slot], preferred_element_type=F32).astype(BF16).astype(F32)
        act = (gate * jax.nn.sigmoid(gate) * up).astype(BF16)
        acc[...] += jnp.dot(act, wd_v[slot], preferred_element_type=F32)

        @pl.when(t + SLOTS < tiles)
        def _():
            for copy in weight_copies(t + SLOTS, slot):
                copy.start()

        return carry

    lax.fori_loop(0, tiles, mlp_step, 0)

    copy_a = send(acc.at[other], got_a, sa.at[0], ta.at[0], core_id)
    copy_a.start()
    copy_a.wait_recv()
    sum_a[...] = acc[mine] + got_a[...]
    zmine = pl.ds(pl.multiple_of(z * 16, 16), 16)
    zother = pl.ds(pl.multiple_of((1 - z) * 16, 16), 16)
    copy_b = send(sum_a.at[zother], got_b, sa.at[1], ta.at[1], z_id)
    copy_b.start()
    copy_b.wait_recv()

    def rows_of(flips, fc=0):
        px = 1 - xx if "x" in flips else xx
        py = 1 - yy if "y" in flips else yy
        pz = 1 - z if "z" in flips else z
        pc = 1 - c if fc else c
        block = ((py * 2 + px) * 2 + pc) * 2 + pz
        return pl.ds(pl.multiple_of(block * 16, 16), 16)

    hid16 = hid[pl.ds(pl.multiple_of(c * 32 + z * 16, 16), 16), :]
    yall[rows_of("")] = (hid16 + (sum_a[zmine] + got_b[...])).astype(BF16).astype(F32)

    ids = {"x": x_id, "y": y_id, "z": z_id}
    orders = ("xyz", "yzx", "zxy")

    def gather_copy(p, idx):
        d0, d1, d2 = orders[p]
        src = ["", "", d0, "", d0, d1, d0 + d1][idx]
        to_dim = [d0, d1, d1, d2, d2, d2, d2][idx]
        ref = yall.at[rows_of(src), pl.ds(*CUTS[p])]
        return send(ref, ref, sg.at[p, idx], tg.at[p, idx], ids[to_dim])

    def landed(p, idx):
        d0, d1, d2 = orders[p]
        return [d0, d1, d0 + d1, d2, d2 + d0, d2 + d1, d0 + d1 + d2][idx]

    def gather_wait(p, idx):
        ref = yall.at[rows_of(landed(p, idx)), pl.ds(*CUTS[p])]
        send(ref, ref, sg.at[p, idx], tg.at[p, idx], core_id).wait_recv()

    def core_copy(p, j):
        flips = "" if j == 0 else landed(p, j - 1)
        ref = yall.at[rows_of(flips), pl.ds(*CUTS[p])]
        return send(ref, ref, sd.at[p, j], td.at[p, j], core_id)

    for idx in (0, 1, 3):
        for p in range(3):
            gather_copy(p, idx).start()
    for p in range(3):
        core_copy(p, 0).start()
    for p in range(3):
        gather_wait(p, 0)
        gather_copy(p, 2).start()
        gather_copy(p, 4).start()
        core_copy(p, 1).start()
    for p in range(3):
        gather_wait(p, 1)
        gather_copy(p, 5).start()
        core_copy(p, 2).start()
    for p in range(3):
        gather_wait(p, 2)
        gather_copy(p, 6).start()
        core_copy(p, 3).start()
    for idx in (3, 4, 5, 6):
        for p in range(3):
            gather_wait(p, idx)
            core_copy(p, idx + 1).start()
    for p in range(3):
        for j in range(8):
            flips = "" if j == 0 else landed(p, j - 1)
            ref = yall.at[rows_of(flips, 1), pl.ds(*CUTS[p])]
            send(ref, ref, sd.at[p, j], td.at[p, j], core_id).wait_recv()
    y_ref[...] = yall[...].astype(BF16)

    for pair in first + second:
        for copy in pair:
            copy.wait_send()
    for copy in (copy_o, copy_z, copy_h, copy_a, copy_b):
        copy.wait_send()
    for p in range(3):
        for idx in range(7):
            gather_copy(p, idx).wait_send()
        for j in range(8):
            core_copy(p, j).wait_send()


def tail(o, ml, x_tok, g_mlp, wo, wg, wu, wd):
    batch, width = x_tok.shape
    depth = wo.shape[0] // 2
    vmem = pl.BlockSpec(memory_space=pltpu.VMEM)
    hbm = pl.BlockSpec(memory_space=pl.ANY)
    dma = pltpu.SemaphoreType.DMA
    heads = (64, 8, 128)
    stat = (2, 8, 128)
    return pl.pallas_call(
        tail_kernel,
        name="tail",
        out_shape=jax.ShapeDtypeStruct((batch, width), BF16),
        in_specs=[vmem, vmem, vmem, vmem, hbm, hbm, hbm, hbm],
        out_specs=vmem,
        scratch_shapes=[
            pltpu.VMEM((4, *heads), F32), pltpu.VMEM((4, *stat), F32),
            pltpu.VMEM((4, *heads), F32), pltpu.VMEM((4, *stat), F32),
            pltpu.VMEM((3, *heads), F32), pltpu.VMEM((3, *stat), F32),
            pltpu.VMEM(heads, F32), pltpu.VMEM((64, depth), BF16),
            pltpu.VMEM((depth, width), BF16), pltpu.VMEM((64, width), F32),
            pltpu.VMEM((32, width), F32), pltpu.VMEM((32, width), F32), pltpu.VMEM((32, width), F32),
            pltpu.VMEM((64, width), F32), pltpu.VMEM((64, width), BF16),
            pltpu.VMEM((SLOTS, width, TILE_F), BF16), pltpu.VMEM((SLOTS, width, TILE_F), BF16), pltpu.VMEM((SLOTS, TILE_F, width), BF16),
            pltpu.VMEM((64, width), F32), pltpu.VMEM((32, width), F32), pltpu.VMEM((32, width), F32), pltpu.VMEM((16, width), F32),
            pltpu.VMEM((batch, width), F32),
            dma, dma((3, SLOTS)), dma((2, 4)), dma((2, 4)), dma((2, 3)), dma((2, 3)),
            dma((3,)), dma((3,)), dma((2,)), dma((2,)), dma((3, 7)), dma((3, 7)), dma((3, 8)), dma((3, 8)),
        ],
        compiler_params=pltpu.CompilerParams(collective_id=0, has_side_effects=True, vmem_limit_bytes=VMEM_LIMIT),
        cost_estimate=pl.CostEstimate(flops=10**10, bytes_accessed=10**8, transcendentals=0),
    )(o, ml, x_tok, g_mlp, wo, wg, wu, wd)


def solution(mesh):
    cache_spec = P(None, "sp", "tp", None)
    col_spec = P(None, "tp")
    row_spec = P("tp", None)
    full_spec = P()

    def local_step(x_tok, seq_lens, k_blk, v_blk, g_attn, wq_loc, wk_loc, wv_loc, wo_loc, g_mlp, wg_loc, wu_loc, wd_loc):
        batch_rows, seq_blk, kv_loc, head_dim = k_blk.shape
        half = head_dim // 2
        inv_freq = jnp.power(F32(ROPE_BASE), jnp.arange(half, dtype=F32) * (-2.0 / head_dim))
        angles = seq_lens.astype(F32)[:, None] * jnp.concatenate([inv_freq, inv_freq])
        cos2 = jnp.cos(angles)
        sin2 = jnp.sin(angles) * jnp.where(jnp.arange(head_dim) < half, -1.0, 1.0)
        pos = seq_lens - lax.axis_index("sp") * seq_blk
        flat = (batch_rows, seq_blk * kv_loc, head_dim)
        k_out, v_out, o, ml = front(
            pos, x_tok, g_attn.reshape(1, -1), cos2, sin2, wq_loc, wk_loc, wv_loc, k_blk.reshape(flat), v_blk.reshape(flat)
        )
        y_out = tail(o, ml, x_tok, g_mlp.reshape(1, -1), wo_loc, wg_loc, wu_loc, wd_loc)
        return y_out, k_out.reshape(k_blk.shape), v_out.reshape(v_blk.shape)

    return jax.shard_map(local_step, mesh=mesh, in_specs=(full_spec, full_spec, cache_spec, cache_spec, full_spec, col_spec, col_spec, col_spec, row_spec, full_spec, col_spec, col_spec, row_spec), out_specs=(full_spec, cache_spec, cache_spec), check_vma=False)
```

```python
import functools

import jax
import jax.numpy as jnp
from jax import lax
from jax.experimental import pallas as pl
from jax.experimental.pallas import tpu as pltpu
from jax.sharding import PartitionSpec as P

ROPE_BASE = 500000.0
NORM_EPS = 1e-5
F32 = jnp.float32
BF16 = jnp.bfloat16
MESH = pl.DeviceIdType.MESH
VMEM_LIMIT = 67_000_000

ROWS_STEP = 16
CHUNK = 512
RING = 6
SLOTS = 20
ORDERS = ("zxy", "yzx", "zxy", "xyz", "zxy", "yzx", "zxy", "yzx")


def front_kernel(pos_ref, x_ref, g_ref, cos_ref, sin_ref, wq_hbm, wk_hbm, wv_hbm, k_hbm, v_hbm,
                 ko_hbm, vo_hbm, o_ref, ml_ref, xn, w_v, qf, kf, vf, kbuf, vbuf, w_sem, in_sem, out_sem):
    batch = x_ref.shape[0]
    rows, dim = k_hbm.shape[1:]
    kv = rows // 64
    heads = wq_hbm.shape[1] // dim
    group = heads // kv
    scale = dim**-0.5
    steps = batch // ROWS_STEP
    q_tiles, k_tiles = wq_hbm.shape[1] // 256, wk_hbm.shape[1] // 256

    weights = [(wq_hbm, j) for j in range(q_tiles)] + [(wk_hbm, j) for j in range(k_tiles)] + [(wv_hbm, j) for j in range(k_tiles)]
    for t, (ref, j) in enumerate(weights):
        pltpu.make_async_copy(ref.at[:, pl.ds(j * 256, 256)], w_v.at[t], w_sem.at[t]).start()

    def block_in(t, slot):
        at = pl.ds(pl.multiple_of(t * ROWS_STEP, ROWS_STEP), ROWS_STEP)
        return (
            pltpu.make_async_copy(k_hbm.at[at], kbuf.at[slot], in_sem.at[0, slot]),
            pltpu.make_async_copy(v_hbm.at[at], vbuf.at[slot], in_sem.at[1, slot]),
        )

    def block_out(t, slot):
        at = pl.ds(pl.multiple_of(t * ROWS_STEP, ROWS_STEP), ROWS_STEP)
        return (
            pltpu.make_async_copy(kbuf.at[slot], ko_hbm.at[at], out_sem.at[0, slot]),
            pltpu.make_async_copy(vbuf.at[slot], vo_hbm.at[at], out_sem.at[1, slot]),
        )

    for t in range(RING):
        for copy in block_in(t, t):
            copy.start()

    def norm_step(j, carry):
        at = pl.ds(pl.multiple_of(j * 32, 32), 32)
        x = x_ref[at, :].astype(F32)
        r = lax.rsqrt(jnp.mean(x * x, axis=-1, keepdims=True) + NORM_EPS)
        xn[at, :] = (x * r * g_ref[0:1, :]).astype(BF16)
        return carry

    lax.fori_loop(0, batch // 32, norm_step, 0)

    def project(t):
        pltpu.make_async_copy(wk_hbm.at[:, pl.ds(0, 256)], w_v.at[t], w_sem.at[t]).wait()
        return jnp.dot(xn[...], w_v[t], preferred_element_type=F32).astype(BF16).astype(F32)

    def rotate(head):
        return (head * cos_ref[...] + pltpu.roll(head, dim // 2, 1) * sin_ref[...]).astype(BF16).astype(F32)

    def q_step(t, carry):
        y = project(t)
        for j in range(2):
            qf[pl.ds(2 * t + j, batch, stride=heads), :] = rotate(y[:, j * dim : (j + 1) * dim])
        return carry

    def k_step(t, carry):
        y = project(q_tiles + t)
        for j in range(2):
            head = rotate(y[:, j * dim : (j + 1) * dim])
            for rep in range(16 // kv):
                kf[pl.ds(rep * kv + 2 * t + j, batch, stride=16), :] = head
        return carry

    def v_step(t, carry):
        y = project(q_tiles + k_tiles + t)
        for j in range(2):
            for rep in range(16 // kv):
                vf[pl.ds(rep * kv + 2 * t + j, batch, stride=16), :] = y[:, j * dim : (j + 1) * dim]
        return carry

    lax.fori_loop(0, q_tiles, q_step, 0)
    lax.fori_loop(0, k_tiles, k_step, 0)
    lax.fori_loop(0, k_tiles, v_step, 0)

    ml_ref[...] = jnp.zeros_like(ml_ref)
    row16 = lax.broadcasted_iota(jnp.int32, (16, dim), 0)
    row_id = lax.broadcasted_iota(jnp.int32, (heads, rows), 0)
    col_id = lax.broadcasted_iota(jnp.int32, (heads, rows), 1)
    same_head = (col_id % kv) == (row_id // group)
    col_id = jnp.where(same_head, col_id, rows * 1024)
    lane = lax.broadcasted_iota(jnp.int32, (heads, 128), 1)
    per = 64 // ROWS_STEP

    def attend_step(t, carry):
        slot = lax.rem(t, RING)
        chip, part = lax.div(t, per), lax.rem(t, per)
        for copy in block_in(t, slot):
            copy.wait()
        for b in range(ROWS_STEP):
            first = pos_ref[t * ROWS_STEP + b] * kv
            start = pl.multiple_of(jnp.clip(first // 16, 0, rows // 16 - 1) * 16, 16)
            lo = first - start
            here = (row16 >= lo) & (row16 < lo + kv)
            new = pl.ds(pl.multiple_of((t * ROWS_STEP + b) * 16, 16), 16)
            at = pl.ds(start, 16)
            kbuf[slot, b, at, :] = jnp.where(here, kf[new, :].astype(BF16), kbuf[slot, b, at, :])
            vbuf[slot, b, at, :] = jnp.where(here, vf[new, :].astype(BF16), vbuf[slot, b, at, :])
        maxes = jnp.concatenate([ml_ref[chip, 0, 0], ml_ref[chip, 1, 0]], axis=0)
        sums = jnp.concatenate([ml_ref[chip, 0, 1], ml_ref[chip, 1, 1]], axis=0)
        for base in range(0, ROWS_STEP, 8):
            scores, weights = [], []
            for b in range(base, base + 8):
                q = qf[pl.ds(pl.multiple_of((t * ROWS_STEP + b) * heads, heads), heads), :].astype(BF16)
                s = lax.dot_general(q, kbuf[slot, b], (((1,), (1,)), ((), ())), preferred_element_type=F32)
                scores.append(s * scale)
            for n, b in enumerate(range(base, base + 8)):
                valid = col_id < (pos_ref[t * ROWS_STEP + b] + 1) * kv
                s = jnp.where(valid, scores[n], -1e30)
                m = jnp.max(s, axis=1, keepdims=True)
                w = jnp.where(valid, jnp.exp(s - m), 0.0)
                here = lane == part * ROWS_STEP + b
                maxes = jnp.where(here, m, maxes)
                sums = jnp.where(here, jnp.sum(w, axis=1, keepdims=True), sums)
                weights.append(w.astype(BF16))
            for n, b in enumerate(range(base, base + 8)):
                o = jnp.dot(weights[n], vbuf[slot, b], preferred_element_type=F32)
                o_ref[chip, 0, part * ROWS_STEP + b] = o[:8]
                o_ref[chip, 1, part * ROWS_STEP + b] = o[8:]
        ml_ref[chip, 0, 0] = maxes[:8]
        ml_ref[chip, 1, 0] = maxes[8:]
        ml_ref[chip, 0, 1] = sums[:8]
        ml_ref[chip, 1, 1] = sums[8:]
        for copy in block_out(t, slot):
            copy.start()

        @pl.when((t >= 1) & (t - 1 + RING < steps))
        def _():
            before = lax.rem(t - 1, RING)
            for copy in block_out(t - 1, before):
                copy.wait()
            for copy in block_in(t - 1 + RING, before):
                copy.start()

        return carry

    lax.fori_loop(0, steps, attend_step, 0)
    for t in range(steps - RING, steps):
        for copy in block_out(t, t % RING):
            copy.wait()


def front(pos, x_tok, g_attn, cos2, sin2, wq, wk, wv, k_blk, v_blk):
    batch, width = x_tok.shape
    _, rows, dim = k_blk.shape
    heads = wq.shape[1] // dim
    tiles = (wq.shape[1] + wk.shape[1] + wv.shape[1]) // 256
    vmem = pl.BlockSpec(memory_space=pltpu.VMEM)
    hbm = pl.BlockSpec(memory_space=pl.ANY)
    dma = pltpu.SemaphoreType.DMA
    return pl.pallas_call(
        front_kernel,
        name="front",
        in_specs=[pl.BlockSpec(memory_space=pltpu.SMEM), vmem, vmem, vmem, vmem, hbm, hbm, hbm, hbm, hbm],
        out_specs=[hbm, hbm, vmem, vmem],
        out_shape=[
            jax.ShapeDtypeStruct(k_blk.shape, BF16),
            jax.ShapeDtypeStruct(v_blk.shape, BF16),
            jax.ShapeDtypeStruct((batch // 64, 2, 64, 8, dim), F32),
            jax.ShapeDtypeStruct((batch // 64, 2, 2, 8, dim), F32),
        ],
        scratch_shapes=[
            pltpu.VMEM((batch, width), BF16),
            pltpu.VMEM((tiles, width, 256), BF16),
            pltpu.VMEM((batch * heads, dim), F32), pltpu.VMEM((batch * 16, dim), F32), pltpu.VMEM((batch * 16, dim), F32),
            pltpu.VMEM((RING, ROWS_STEP, rows, dim), BF16), pltpu.VMEM((RING, ROWS_STEP, rows, dim), BF16),
            dma((tiles,)), dma((2, RING)), dma((2, RING)),
        ],
        compiler_params=pltpu.CompilerParams(vmem_limit_bytes=VMEM_LIMIT),
        cost_estimate=pl.CostEstimate(flops=10**10, bytes_accessed=10**8, transcendentals=0),
    )(pos, x_tok, g_attn, cos2, sin2, wq, wk, wv, k_blk, v_blk)


def blend(first, count, pairs, out_ref):
    for b in range(count):
        total = None
        for weight, part in pairs:
            term = jnp.broadcast_to(weight[:, first + b : first + b + 1], (8, 128)) * part[b]
            total = term if total is None else total + term
        out_ref[b] = total


def tail_kernel(o_ref, ml_ref, g_ref, x_hbm, wo_hbm, wg_hbm, wu_hbm, wd_hbm, y_ref,
                r1, rm1, snd, sndm, r2, rm2, attn, attn_bf, part_o, got_o, sum_o, got_z, x_rows, hid, zb,
                ring, act, acc, got_a, sum_a, got_b, yall,
                x_sem, wo_sem, w_sem, s1, t1, s1m, t1m, s2, t2, s2m, t2m, so, to, sz, tz, sh, th, sa, ta, sb, tb, sg, tg, sd, td):
    sp = lax.axis_index("sp")
    z = lax.axis_index("tp")
    c = sp % 2
    xx = (sp // 2) % 2
    yy = sp // 4
    chip = sp // 2
    depth = attn_bf.shape[1]
    model = acc.shape[1]
    width = act.shape[1]
    tiles, pieces = width // 256, model // 256
    first_item = pieces * depth // ring.shape[1]

    def wo_copy(j):
        src = wo_hbm.at[pl.ds(pl.multiple_of(c * depth, depth), depth), pl.ds(j * 256, 256)]
        per = ring.shape[1] // depth
        return pltpu.make_async_copy(src, ring.at[j // per, pl.ds((j % per) * depth, depth)], wo_sem.at[j])

    def up_copy(hbm, t, slot):
        at = pl.ds(pl.multiple_of(c * width + t * 256, 256), 256)
        return pltpu.make_async_copy(hbm.at[:, at], ring.at[slot], w_sem.at[slot])

    def down_copy(j, slot):
        src = wd_hbm.at[pl.ds(pl.multiple_of(c * width, width), width), pl.ds(pl.multiple_of(j * 256, 256), 256)]
        return pltpu.make_async_copy(src, ring.at[slot, pl.ds(0, width)], w_sem.at[slot])

    for j in range(pieces):
        wo_copy(j).start()
    for n in range(first_item, SLOTS):
        up_copy(wu_hbm if (n - first_item) % 2 else wg_hbm, (n - first_item) // 2, n).start()
    x_copies = []
    for half in range(2):
        at = pl.ds(pl.multiple_of(chip * 64 + half * 32 + c * 16, 16), 16)
        x_copies.append(pltpu.make_async_copy(x_hbm.at[at, :], x_rows.at[half], x_sem.at[half]))
        x_copies[half].start()

    def spi(fx, fy, fc):
        px = 1 - xx if fx else xx
        py = 1 - yy if fy else yy
        pc = 1 - c if fc else c
        return (py * 2 + px) * 2 + pc

    core_id = {"sp": spi(0, 0, 1)}
    x_id = {"sp": spi(1, 0, 0)}
    y_id = {"sp": spi(0, 1, 0)}
    d_id = {"sp": spi(1, 1, 0)}
    z_id = {"tp": 1 - z}

    barrier = pltpu.get_barrier_semaphore()
    for peer in (core_id, x_id, y_id, d_id, z_id):
        pl.semaphore_signal(barrier, inc=1, device_id=peer, device_id_type=MESH)
    pl.semaphore_wait(barrier, 5)

    sent = []

    def send(src, dst, send_sem, recv_sem, peer):
        copy = pltpu.make_async_remote_copy(src_ref=src, dst_ref=dst, send_sem=send_sem, recv_sem=recv_sem, device_id=peer, device_id_type=MESH)
        copy.start()
        sent.append(copy)
        return copy

    groups = [(1 - yy) * 2 + (1 - xx), yy * 2 + (1 - xx), (1 - yy) * 2 + xx, chip]
    peers = [d_id, x_id, y_id]
    first, stats = {}, []
    for half in range(2):
        rows = pl.ds(half * 32, 32)
        for k in range(4):
            if half == 0:
                stats.append(send(ml_ref.at[groups[k], 1 - c], rm1.at[k], s1m.at[k], t1m.at[k], core_id))
            first[half, k] = send(o_ref.at[groups[k], 1 - c, rows], r1.at[k, rows], s1.at[half, k], t1.at[half, k], core_id)
    second, stats2, factors = {}, [], []
    for half in range(2):
        rows = pl.ds(half * 32, 32)
        for k in range(4):
            if half == 0:
                stats[k].wait_recv()
                m0, m1 = ml_ref[groups[k], c, 0], rm1[k, 0]
                m = jnp.maximum(m0, m1)
                f0, f1 = jnp.exp(m0 - m), jnp.exp(m1 - m)
                factors.append((f0, f1))
                sndm[k, 0] = m
                sndm[k, 1] = f0 * ml_ref[groups[k], c, 1] + f1 * rm1[k, 1]
                if k < 3:
                    stats2.append(send(sndm.at[k], rm2.at[k], s2m.at[k], t2m.at[k], peers[k]))
            first[half, k].wait_recv()
            f0, f1 = factors[k]
            blend(half * 32, 32, [(f0, o_ref.at[groups[k], c, rows]), (f1, r1.at[k, rows])], snd.at[k, rows])
            if k < 3:
                second[half, k] = send(snd.at[k, rows], r2.at[k, rows], s2.at[half, k], t2.at[half, k], peers[k])

    to_z, shares = [], None
    for half in range(2):
        rows = pl.ds(half * 32, 32)
        if half == 0:
            for k in range(3):
                stats2[k].wait_recv()
            ms = [sndm[3, 0]] + [rm2[k, 0] for k in range(3)]
            m = functools.reduce(jnp.maximum, ms)
            fs = [jnp.exp(v - m) for v in ms]
            total = fs[0] * sndm[3, 1] + fs[1] * rm2[0, 1] + fs[2] * rm2[1, 1] + fs[3] * rm2[2, 1]
            total = jnp.where(total > 0.0, total, 1.0)
            shares = [f / total for f in fs]
        for k in (1, 2, 0):
            second[half, k].wait_recv()
        blend(half * 32, 32, [(shares[0], snd.at[3, rows])] + [(shares[k + 1], r2.at[k, rows]) for k in range(3)], attn)
        for h in range(8):
            attn_bf[:, h * 128 : (h + 1) * 128] = attn[:, h, :].astype(BF16)
        if half == 0:
            for j in range(pieces):
                wo_copy(j).wait()
        per = ring.shape[1] // depth

        def wo_step(n, carry):
            for k in range(per):
                at = pl.ds(pl.multiple_of((n * per + k) * 256, 256), 256)
                part_o[half, :, at] = jnp.dot(attn_bf[...], ring[n, k * depth : (k + 1) * depth, :], preferred_element_type=F32)
            return carry

        lax.fori_loop(0, first_item, wo_step, 0)
        mine = pl.ds(pl.multiple_of(c * 16, 16), 16)
        other = pl.ds(pl.multiple_of((1 - c) * 16, 16), 16)
        copy = send(part_o.at[half, other], got_o.at[half], so.at[half], to.at[half], core_id)
        if half == 1:
            for n in range(SLOTS, SLOTS + first_item):
                up_copy(wu_hbm if (n - first_item) % 2 else wg_hbm, (n - first_item) // 2, n - SLOTS).start()
        copy.wait_recv()
        sum_o[half] = part_o[half, mine] + got_o[half]
        to_z.append(send(sum_o.at[half], got_z.at[half], sz.at[half], tz.at[half], z_id))
    to_core = []
    for half in range(2):
        to_z[half].wait_recv()
        x_copies[half].wait()
        hid[half, c] = (x_rows[half].astype(F32) + (sum_o[half] + got_z[half])).astype(BF16).astype(F32)
        to_core.append(send(hid.at[half, c], hid.at[half, c], sh.at[half], th.at[half], core_id))
    for half in range(2):
        to_core[half].wait_recv()

    for cc in range(2):
        for zz in range(2):
            h = jnp.concatenate([hid[0, cc, zz * 8 : zz * 8 + 8, :], hid[1, cc, zz * 8 : zz * 8 + 8, :]], axis=0)
            r = lax.rsqrt(jnp.mean(h * h, axis=-1, keepdims=True) + NORM_EPS)
            zb[(cc * 2 + zz) * 16 : (cc * 2 + zz) * 16 + 16, :] = (h * r * g_ref[1:2, :]).astype(BF16)

    def up_step(t, carry):
        n = first_item + 2 * t
        slots = [lax.rem(n, SLOTS), lax.rem(n + 1, SLOTS)]
        up_copy(wg_hbm, t, slots[0]).wait()
        gate = jnp.dot(zb[...], ring[slots[0]], preferred_element_type=F32).astype(BF16).astype(F32)
        up_copy(wu_hbm, t, slots[1]).wait()
        up = jnp.dot(zb[...], ring[slots[1]], preferred_element_type=F32).astype(BF16).astype(F32)
        act[:, pl.ds(pl.multiple_of(t * 256, 256), 256)] = (gate * jax.nn.sigmoid(gate) * up).astype(BF16)
        later = n + SLOTS - first_item

        @pl.when(later < 2 * tiles)
        def _():
            up_copy(wg_hbm, later // 2, slots[0]).start()
            up_copy(wu_hbm, later // 2, slots[1]).start()

        @pl.when((later >= 2 * tiles) & (later < 2 * tiles + pieces))
        def _():
            down_copy(later - 2 * tiles, slots[0]).start()
            down_copy(later + 1 - 2 * tiles, slots[1]).start()

        return carry

    lax.fori_loop(0, tiles, up_step, 0)

    mine = pl.ds(pl.multiple_of(c * 32, 32), 32)
    other = pl.ds(pl.multiple_of((1 - c) * 32, 32), 32)
    zmine = pl.ds(pl.multiple_of(z * 16, 16), 16)
    zother = pl.ds(pl.multiple_of((1 - z) * 16, 16), 16)
    ids = {"x": x_id, "y": y_id, "z": z_id}

    def rows_of(flips):
        px = 1 - xx if "x" in flips else xx
        py = 1 - yy if "y" in flips else yy
        pz = 1 - z if "z" in flips else z
        block = ((py * 2 + px) * 2 + c) * 2 + pz
        return pl.ds(pl.multiple_of(block * 16, 16), 16)

    def columns(n):
        return pl.ds(n * CHUNK, CHUNK)

    def gather_send(n, idx):
        d0, d1, d2 = ORDERS[n]
        src = ["", "", d0, "", d0, d1, d0 + d1][idx]
        along = [d0, d1, d1, d2, d2, d2, d2][idx]
        ref = yall.at[rows_of(src), columns(n)]
        gathers.append(pltpu.make_async_remote_copy(src_ref=ref, dst_ref=ref, send_sem=sg.at[n, idx], recv_sem=tg.at[n, idx], device_id=ids[along], device_id_type=MESH))
        gathers[-1].start()

    def landed(n, idx):
        d0, d1, d2 = ORDERS[n]
        return [d0, d1, d0 + d1, d2, d2 + d0, d2 + d1, d0 + d1 + d2][idx]

    def core_send(n, j):
        ref = yall.at[rows_of("" if j == 0 else landed(n, j - 1)), columns(n)]
        gathers.append(pltpu.make_async_remote_copy(src_ref=ref, dst_ref=ref, send_sem=sd.at[n, j], recv_sem=td.at[n, j], device_id=core_id, device_id_type=MESH))
        gathers[-1].start()

    def gather_wait(n, idx):
        ref = yall.at[rows_of(landed(n, idx)), columns(n)]
        pltpu.make_async_remote_copy(src_ref=ref, dst_ref=ref, send_sem=sg.at[n, idx], recv_sem=tg.at[n, idx], device_id=core_id, device_id_type=MESH).wait_recv()

    def core_wait(n, j):
        ref = yall.at[rows_of(""), columns(n)]
        pltpu.make_async_remote_copy(src_ref=ref, dst_ref=ref, send_sem=sd.at[n, j], recv_sem=td.at[n, j], device_id=core_id, device_id_type=MESH).wait_recv()

    gathers, to_a, to_b = [], {}, {}
    chunks = model // CHUNK
    per = CHUNK // 256

    def stage0(n):
        for k in range(per):
            j = n * per + k
            item = first_item + 2 * tiles + j
            slot = item % SLOTS
            down_copy(j, slot).wait()
            acc[:, j * 256 : (j + 1) * 256] = jnp.dot(act[...], ring[slot, 0:width, :], preferred_element_type=F32)
            later = item + SLOTS - first_item - 2 * tiles
            if later < pieces:
                down_copy(later, slot).start()
        to_a[n] = send(acc.at[other, columns(n)], got_a.at[:, columns(n)], sa.at[n], ta.at[n], core_id)

    def stage1(n):
        to_a[n].wait_recv()
        sum_a[:, columns(n)] = acc[mine, columns(n)] + got_a[:, columns(n)]
        to_b[n] = send(sum_a.at[zother, columns(n)], got_b.at[:, columns(n)], sb.at[n], tb.at[n], z_id)

    def stage2(n):
        to_b[n].wait_recv()
        own = pl.ds(pl.multiple_of(z * 8, 8), 8)
        h = jnp.concatenate([hid[0, c, own, columns(n)], hid[1, c, own, columns(n)]], axis=0)
        yall[rows_of(""), columns(n)] = (h + (sum_a[zmine, columns(n)] + got_b[:, columns(n)])).astype(BF16).astype(F32)
        for idx in (0, 1, 3):
            gather_send(n, idx)
        core_send(n, 0)

    def stage3(n):
        gather_wait(n, 0)
        gather_send(n, 2)
        gather_send(n, 4)
        core_send(n, 1)
        gather_wait(n, 1)
        gather_send(n, 5)
        core_send(n, 2)

    def stage4(n):
        gather_wait(n, 2)
        gather_send(n, 6)
        core_send(n, 3)

    def stage5(n):
        for idx in (3, 4, 5, 6):
            gather_wait(n, idx)
            core_send(n, idx + 1)

    def stage6(n):
        for j in range(8):
            core_wait(n, j)

    for n in range(chunks + 6):
        for stage, lag in ((stage0, 0), (stage1, 1), (stage2, 2), (stage3, 3), (stage4, 4), (stage5, 5), (stage6, 6)):
            if 0 <= n - lag < chunks:
                stage(n - lag)

    def finish(g, carry):
        block = lax.div(g, 4) * 4 + lax.rem(g, 2) * 2
        half = lax.rem(lax.div(g, 2), 2)
        parts = [yall[pl.ds(pl.multiple_of((block + zz) * 16 + half * 8, 8), 8), :] for zz in range(2)]
        y_ref[pl.ds(pl.multiple_of(g * 16, 16), 16), :] = jnp.concatenate(parts, axis=0).astype(BF16)
        return carry

    lax.fori_loop(0, y_ref.shape[0] // 16, finish, 0)
    for copy in sent + gathers:
        copy.wait_send()


def tail(o, ml, gains, x_tok, wo, wg, wu, wd):
    batch, width = x_tok.shape
    depth = wo.shape[0] // 2
    quarter = wg.shape[1] // 2
    vmem = pl.BlockSpec(memory_space=pltpu.VMEM)
    hbm = pl.BlockSpec(memory_space=pl.ANY)
    dma = pltpu.SemaphoreType.DMA
    heads = (64, 8, 128)
    stat = (2, 8, 128)
    chunks = width // CHUNK
    return pl.pallas_call(
        tail_kernel,
        name="tail",
        out_shape=jax.ShapeDtypeStruct((batch, width), BF16),
        in_specs=[vmem, vmem, vmem, hbm, hbm, hbm, hbm, hbm],
        out_specs=vmem,
        scratch_shapes=[
            pltpu.VMEM((4, *heads), F32), pltpu.VMEM((4, *stat), F32),
            pltpu.VMEM((4, *heads), F32), pltpu.VMEM((4, *stat), F32),
            pltpu.VMEM((3, *heads), F32), pltpu.VMEM((3, *stat), F32),
            pltpu.VMEM((32, 8, 128), F32), pltpu.VMEM((32, depth), BF16),
            pltpu.VMEM((2, 32, width), F32), pltpu.VMEM((2, 16, width), F32), pltpu.VMEM((2, 16, width), F32), pltpu.VMEM((2, 16, width), F32),
            pltpu.VMEM((2, 16, width), BF16), pltpu.VMEM((2, 2, 16, width), F32), pltpu.VMEM((64, width), BF16),
            pltpu.VMEM((SLOTS, width, 256), BF16), pltpu.VMEM((64, quarter), BF16),
            pltpu.VMEM((64, width), F32), pltpu.VMEM((32, width), F32), pltpu.VMEM((32, width), F32), pltpu.VMEM((16, width), F32),
            pltpu.VMEM((batch, width), F32),
            dma((2,)), dma((width // 256,)), dma((SLOTS,)),
            dma((2, 4)), dma((2, 4)), dma((4,)), dma((4,)), dma((2, 3)), dma((2, 3)), dma((3,)), dma((3,)),
            dma((2,)), dma((2,)), dma((2,)), dma((2,)), dma((2,)), dma((2,)),
            dma((chunks,)), dma((chunks,)), dma((chunks,)), dma((chunks,)),
            dma((chunks, 7)), dma((chunks, 7)), dma((chunks, 8)), dma((chunks, 8)),
        ],
        compiler_params=pltpu.CompilerParams(collective_id=0, has_side_effects=True, vmem_limit_bytes=VMEM_LIMIT),
        cost_estimate=pl.CostEstimate(flops=10**10, bytes_accessed=10**8, transcendentals=0),
    )(o, ml, gains, x_tok, wo, wg, wu, wd)


def solution(mesh):
    cache_spec = P(None, "sp", "tp", None)
    col_spec = P(None, "tp")
    row_spec = P("tp", None)
    full_spec = P()

    def local_step(x_tok, seq_lens, k_blk, v_blk, g_attn, wq_loc, wk_loc, wv_loc, wo_loc, g_mlp, wg_loc, wu_loc, wd_loc):
        batch_rows, seq_blk, kv_loc, head_dim = k_blk.shape
        gains = jnp.stack([g_attn, g_mlp]).astype(F32)
        half = head_dim // 2
        inv_freq = jnp.power(F32(ROPE_BASE), jnp.arange(half, dtype=F32) * (-2.0 / head_dim))
        angles = seq_lens.astype(F32)[:, None] * jnp.concatenate([inv_freq, inv_freq])
        cos2 = jnp.cos(angles)
        sin2 = jnp.sin(angles) * jnp.where(jnp.arange(head_dim) < half, -1.0, 1.0)
        pos = seq_lens - lax.axis_index("sp") * seq_blk
        flat = (batch_rows, seq_blk * kv_loc, head_dim)
        k_out, v_out, o, ml = front(
            pos, x_tok, gains, cos2, sin2, wq_loc, wk_loc, wv_loc, k_blk.reshape(flat), v_blk.reshape(flat)
        )
        y_out = tail(o, ml, gains, x_tok, wo_loc, wg_loc, wu_loc, wd_loc)
        return y_out, k_out.reshape(k_blk.shape), v_out.reshape(v_blk.shape)

    return jax.shard_map(local_step, mesh=mesh, in_specs=(full_spec, full_spec, cache_spec, cache_spec, full_spec, col_spec, col_spec, col_spec, row_spec, full_spec, col_spec, col_spec, row_spec), out_specs=(full_spec, cache_spec, cache_spec), check_vma=False)
```
